32 devices in a mesh: px: 2 (over core), py: 4 (over z), ta: 4 (over y, x).
Axes of the slice: x: 2, y: 2, z: 4, core: 2. Of those that a mesh axis runs over, the one named last changes fastest.
Arguments:
- snapshots: bfloat16 [384, 5, 65536], P('ta', None, ('px', 'py')), may hold values from -6 to 6
- quad_weights: float32 [65536], P(('px', 'py')), may hold values from 1 to 10
- spectral_indices: int32 [32], replicated, may hold values from 0 to 127
Outputs:
- spectra: float32 [32, 2, 2, 5, 65536], P('ta', None, None, None, ('px', 'py'))
- gram: float32 [32, 2, 2, 2], P('ta')
The draws below stay inside these ranges and needn't reach their ends.
All inputs are finite; a program needn't handle non-finite values.
Results may differ from the reference program's by a relative error of at most 0.0042.
Values may be sent and summed in bfloat16 or wider, within the bound.
A program may use at most 128 MiB of HBM per device.

```python
import math
import jax
import jax.numpy as jnp
from jax import lax

VARS = 5
BLK = 256
HOP = 128
SEGMENT_NUMBER = 2
RECORD_LENGTH = 384
RETAINED_MODES = 32
POINTS = 65536


def place_ends(values, key, least, high):
    index_at = [jax.random.randint(jax.random.fold_in(key, axis), (), 0, length) for axis, length in enumerate(values.shape)]
    widest = values.shape.index(max(values.shape))
    beside = index_at[:widest] + [(index_at[widest] + 1) % values.shape[widest]] + index_at[widest + 1:]
    return values.at[tuple(index_at)].set(least).at[tuple(beside)].set(high)


def block_levels(key, dims, cuts, low, top_value):
    def one(axis_at, parts):
        draws = jax.random.uniform(jax.random.fold_in(jax.random.fold_in(key, 6), axis_at), (parts,), jnp.float32, low / len(cuts), top_value / len(cuts))
        return jnp.repeat(jnp.exp(draws), dims[axis_at] // parts).reshape((-1,) + (1,) * (len(dims) - axis_at - 1))

    loudness = one(*cuts[0])
    for cut in cuts[1:]:
        loudness = loudness * one(*cut)
    return loudness


def scatter_about(rng, dims, spread, most, pieces=(), kind=jnp.bfloat16):
    loudness = block_levels(rng, dims, pieces, -0.22, 0.18) if pieces else 1.0
    entries = jax.random.normal(rng, dims, jnp.float32) * spread * loudness
    return jnp.minimum(jnp.maximum(entries, -most), most).astype(kind)


def setup_inputs(seed: int = 0) -> dict:
    key_list = jax.random.split(jax.random.key(seed), 4)
    return {
        "snapshots": scatter_about(key_list[0], (RECORD_LENGTH, VARS, POINTS), 1.0, 6.0, ((0, 4), (2, 8))),
        "quad_weights": jnp.clip(jnp.exp(math.log(10.0) - 2.3025851 * jax.random.uniform(key_list[1], (POINTS,), jnp.float32) ** block_levels(key_list[1], (POINTS,), ((0, 8),), -0.2, 0.2)), 1.0, 10.0),
        "spectral_indices": place_ends(jax.random.randint(key_list[2], (RETAINED_MODES,), 0, BLK // 2), jax.random.fold_in(key_list[2], 1), 0, (BLK // 2) - 1).astype(jnp.int32),
    }


def make_rotation_multipliers(spectral_indices, temporal_locations):
    segment_beginnings = jnp.arange(SEGMENT_NUMBER, dtype=jnp.int32) * HOP
    segment_shifts = temporal_locations[None, :] - segment_beginnings[:, None]
    inside = (segment_shifts >= 0) & (segment_shifts < BLK)
    window = 0.5 - 0.5 * jnp.cos(2.0 * math.pi * segment_shifts.astype(jnp.float32) / BLK)
    window = jnp.where(inside, window, jnp.float32(0.0)) / jnp.sqrt(jnp.float32(3.0 * BLK / 8.0))
    phases = jnp.mod(spectral_indices[:, None, None] * segment_shifts[None, :, :], BLK)
    angles = 2.0 * math.pi * phases.astype(jnp.float32) / BLK
    real_part = jnp.cos(angles) * window[None]
    imag_part = -jnp.sin(angles) * window[None]
    gathered_segments = jnp.stack([real_part, imag_part], axis=2)
    return gathered_segments.reshape(RETAINED_MODES * SEGMENT_NUMBER * 2, temporal_locations.shape[0]).astype(jnp.bfloat16)

def gram_terms(spectra):
    flat = spectra.reshape(spectra.shape[0], 2 * SEGMENT_NUMBER, -1)
    inner = jnp.einsum('fam,fbm->fab', flat, flat, precision=lax.Precision.HIGHEST)
    inner = inner.reshape(spectra.shape[0], SEGMENT_NUMBER, 2, SEGMENT_NUMBER, 2)
    real_part = inner[:, :, 0, :, 0] + inner[:, :, 1, :, 1]
    imag_part = inner[:, :, 0, :, 1] - inner[:, :, 1, :, 0]
    return jnp.stack([real_part, imag_part], axis=-1)

def reference(snapshots, quad_weights, spectral_indices):
    temporal_locations = jnp.arange(RECORD_LENGTH, dtype=jnp.int32)
    rotation_multipliers = make_rotation_multipliers(spectral_indices, temporal_locations)
    flat_snapshots = snapshots.reshape(RECORD_LENGTH, VARS * POINTS)
    raw = jnp.dot(rotation_multipliers, flat_snapshots, preferred_element_type=jnp.float32)
    raw = raw.reshape(RETAINED_MODES, SEGMENT_NUMBER, 2, VARS, POINTS)
    spectra = raw * jnp.sqrt(quad_weights)
    gram = gram_terms(spectra) / jnp.float32(POINTS * VARS)
    return (spectra, gram)
```

```python
import functools
import math

import jax
import jax.numpy as jnp
from jax import lax
from jax.experimental import pallas as pl
from jax.experimental.pallas import tpu as pltpu
from jax.sharding import PartitionSpec as P

VARS = 5
BLK = 256
HOP = 128
SEGMENT_NUMBER = 2
RETAINED_MODES = 32

MESH = pl.DeviceIdType.MESH
HALF_NEIGHBOUR = (1, 2)
POSITIONS = (0, 1, 3, 2)
SENT_AT = ((1, 2), (2, 3))
PASSED_AT = (3, 1)
RECEIVED = ((0, 1), (1, 0))


def make_rotation_multipliers(spectral_indices, temporal_locations):
    segment_beginnings = jnp.arange(SEGMENT_NUMBER, dtype=jnp.int32) * HOP
    segment_shifts = temporal_locations[None, :] - segment_beginnings[:, None]
    inside = (segment_shifts >= 0) & (segment_shifts < BLK)
    window = 0.5 - 0.5 * jnp.cos(2.0 * math.pi * segment_shifts.astype(jnp.float32) / BLK)
    window = jnp.where(inside, window, jnp.float32(0.0)) / jnp.sqrt(jnp.float32(3.0 * BLK / 8.0))
    phases = jnp.mod(spectral_indices[:, None, None] * segment_shifts[None, :, :], BLK)
    angles = 2.0 * math.pi * phases.astype(jnp.float32) / BLK
    real_part = jnp.cos(angles) * window[None]
    imag_part = -jnp.sin(angles) * window[None]
    gathered_segments = jnp.stack([real_part, imag_part], axis=2)
    return gathered_segments.reshape(
        RETAINED_MODES * SEGMENT_NUMBER * 2, temporal_locations.shape[0]
    ).astype(jnp.bfloat16)


def gram_terms(spectra):
    flat = spectra.reshape(spectra.shape[0], 2 * SEGMENT_NUMBER, -1)
    inner = jnp.einsum("fam,fbm->fab", flat, flat, precision=lax.Precision.HIGHEST)
    inner = inner.reshape(spectra.shape[0], SEGMENT_NUMBER, 2, SEGMENT_NUMBER, 2)
    real_part = inner[:, :, 0, :, 0] + inner[:, :, 1, :, 1]
    imag_part = inner[:, :, 0, :, 1] - inner[:, :, 1, :, 0]
    return jnp.stack([real_part, imag_part], axis=-1)


def plain_on_device(snapshots, quad_weights, spectral_indices):
    record_length = snapshots.shape[0]
    point_count = snapshots.shape[2]
    groups = lax.axis_size("ta")
    temporal_locations = lax.axis_index("ta") * record_length + jnp.arange(
        record_length, dtype=jnp.int32
    )
    rotation_multipliers = make_rotation_multipliers(spectral_indices, temporal_locations)
    flat_snapshots = snapshots.reshape(record_length, VARS * point_count)
    raw = lax.psum_scatter(
        jnp.dot(rotation_multipliers, flat_snapshots, preferred_element_type=jnp.float32),
        "ta",
        scatter_dimension=0,
        tiled=True,
    )
    raw = raw.reshape(RETAINED_MODES // groups, SEGMENT_NUMBER, 2, VARS, point_count)
    spectra = raw * jnp.sqrt(quad_weights)
    summed = lax.psum(gram_terms(spectra), ("px", "py"))
    total_points = point_count * lax.axis_size("px") * lax.axis_size("py")
    gram = summed / jnp.float32(total_points * VARS)
    return (spectra, gram)


def window_kernel(
    pieces, width, tile, gram_scale,
    snap_hbm, weight_ref, index_ref, out_hbm, gram_ref,
    snap, twiddle, kept, root, send1, recv1, send2, recv2, out_buf, acc, gram_send, gram_recv,
    load_sem, send1_sem, recv1_sem, send2_sem, recv2_sem, out_sem, gram_send_sem, gram_recv_sem,
):
    px, py, ta = lax.axis_index("px"), lax.axis_index("py"), lax.axis_index("ta")
    npx, npy = lax.axis_size("px"), lax.axis_size("py")
    variables, record, points = snap_hbm.shape
    modes = out_hbm.shape[0]
    unit = 2 * modes
    steps = variables * pieces
    slots = out_buf.shape[0]
    neighbours = [jnp.bitwise_xor(ta, flip) for flip in HALF_NEIGHBOUR]

    def load(variable):
        return pltpu.make_async_copy(snap_hbm.at[variable], snap.at[variable], load_sem.at[variable])

    for variable in range(variables):
        load(variable).start()

    peers = [
        (i, j, lax.rem(px + i, npx), lax.rem(py + j, npy))
        for i in range(npx) for j in range(npy) if i + j > 0
    ]
    barrier = pltpu.get_barrier_semaphore()
    for neighbour in neighbours:
        pl.semaphore_signal(barrier, inc=1, device_id=(px, py, neighbour), device_id_type=MESH)
    for _, _, x, y in peers:
        pl.semaphore_signal(barrier, inc=1, device_id=(x, y, ta), device_id_type=MESH)

    def reaches(group, block):
        first = group * record
        return (first < block * HOP + BLK) & (first + record > block * HOP)

    sublane = lax.broadcasted_iota(jnp.int32, (modes, record), 0)
    moment = lax.broadcasted_iota(jnp.int32, (modes, record), 1) + ta * record
    for position, flip in enumerate(POSITIONS):
        owner = jnp.bitwise_xor(ta, flip)
        bins = jnp.zeros((modes, record), jnp.int32)
        for f in range(modes):
            bins = jnp.where(sublane == f, index_ref[owner * modes + f], bins)
        for block in range(SEGMENT_NUMBER):
            shift = moment - block * HOP
            inside = (shift >= 0) & (shift < BLK)
            hann = 0.5 - 0.5 * jnp.cos((2.0 * math.pi / BLK) * shift.astype(jnp.float32))
            hann = jnp.where(inside, hann, 0.0) / math.sqrt(3.0 * BLK / 8.0)
            angle = (2.0 * math.pi / BLK) * jnp.bitwise_and(bins * shift, BLK - 1).astype(jnp.float32)
            rows = jnp.concatenate([jnp.cos(angle) * hann, -jnp.sin(angle) * hann], axis=0)
            at = (position * SEGMENT_NUMBER + block) * unit
            twiddle[at:at + unit, :] = rows.astype(jnp.bfloat16)
    root[...] = jnp.sqrt(weight_ref[...])
    acc[...] = jnp.zeros_like(acc)

    pl.semaphore_wait(barrier, len(neighbours) + len(peers))

    def target(half):
        return (px, py, neighbours[half])

    def first_copy(half, k, block):
        return pltpu.make_async_remote_copy(
            src_ref=send1.at[half, k, block], dst_ref=recv1.at[half, k, block],
            send_sem=send1_sem.at[half, k, block], recv_sem=recv1_sem.at[half, k, block],
            device_id=target(half), device_id_type=MESH,
        )

    def second_copy(half, k):
        return pltpu.make_async_remote_copy(
            src_ref=send2.at[half, k], dst_ref=recv2.at[half, k],
            send_sem=send2_sem.at[half, k], recv_sem=recv2_sem.at[half, k],
            device_id=target(1 - half), device_id_type=MESH,
        )

    def columns(half, k, at):
        start = lax.rem(k, pieces) * (2 * width) + half * width + at
        return pl.ds(pl.multiple_of(start, 128), tile)

    def transform(k):
        variable = k // pieces

        @pl.when(lax.rem(k, pieces) == 0)
        def _():
            load(variable).wait()

        for half in range(2):
            @pl.loop(0, width // tile)
            def _(i):
                at = pl.multiple_of(i * tile, tile)
                here = pl.ds(at, tile)
                product = jnp.dot(
                    twiddle[...], snap[variable, :, columns(half, k, at)],
                    preferred_element_type=jnp.float32,
                )

                def part(position, block):
                    first = (position * SEGMENT_NUMBER + block) * unit
                    return product[first:first + unit, :]

                for block in range(SEGMENT_NUMBER):
                    for place, position in enumerate(SENT_AT[half]):
                        send1[half, k, block, place * unit:(place + 1) * unit, here] = part(
                            position, block).astype(jnp.bfloat16)
                    kept[half, k, block, 0:unit, here] = part(0, block)
                    kept[half, k, block, unit:2 * unit, here] = part(PASSED_AT[half], block)

            for block in range(SEGMENT_NUMBER):
                @pl.when(reaches(ta, block))
                def _():
                    first_copy(half, k, block).start()

    def pass_on(k):
        for half in range(2):
            own, other = RECEIVED[half]
            for block in range(SEGMENT_NUMBER):
                came = reaches(neighbours[half], block)

                @pl.when(came)
                def _():
                    first_copy(half, k, block).wait_recv()

                @pl.when(jnp.logical_not(came))
                def _():
                    recv1[half, k, block] = jnp.zeros(recv1.shape[3:], jnp.bfloat16)

            @pl.loop(0, width // tile)
            def _(i):
                here = pl.ds(pl.multiple_of(i * tile, tile), tile)
                for block in range(SEGMENT_NUMBER):
                    arrived = recv1[half, k, block, other * unit:(other + 1) * unit, here]
                    total = kept[half, k, block, unit:2 * unit, here] + arrived.astype(jnp.float32)
                    send2[half, k, block * unit:(block + 1) * unit, here] = total.astype(jnp.bfloat16)

            second_copy(half, k).start()

    def write(half, k):
        slot = lax.rem(k, slots)
        start = pl.multiple_of(lax.rem(k, pieces) * (2 * width) + half * width, 128)
        return pltpu.make_async_copy(
            out_buf.at[slot, half],
            out_hbm.at[:, :, k // pieces, :, pl.ds(start, width)],
            out_sem.at[slot, half],
        )

    def finish(k):
        slot = lax.rem(k, slots)
        for half in range(2):
            own, _ = RECEIVED[half]

            @pl.when(k >= slots)
            def _():
                write(half, k - slots).wait()

            second_copy(half, k).wait_recv()

            @pl.loop(0, width // tile)
            def _(i):
                at = pl.multiple_of(i * tile, tile)
                here = pl.ds(at, tile)
                weight = root[:, columns(half, k, at)]
                parts = []
                for block in range(SEGMENT_NUMBER):
                    first = recv1[half, k, block, own * unit:(own + 1) * unit, here]
                    second = recv2[half, k, block * unit:(block + 1) * unit, here]
                    total = kept[half, k, block, 0:unit, here] + (
                        first.astype(jnp.float32) + second.astype(jnp.float32))
                    total = total * weight
                    parts.append((total[:modes], total[modes:]))
                    out_buf[slot, half, :, block, 0, here] = total[:modes]
                    out_buf[slot, half, :, block, 1, here] = total[modes:]
                (r0, i0), (r1, i1) = parts
                terms = (r0 * r0 + i0 * i0, r1 * r1 + i1 * i1, r0 * r1 + i0 * i1, r0 * i1 - i0 * r1)
                for n, term in enumerate(terms):
                    lanes = [term[:, c:c + 128] for c in range(0, tile, 128)]
                    acc[n] += functools.reduce(jnp.add, lanes)

            write(half, k).start()

    ahead = min(2, steps)

    @pl.loop(0, ahead)
    def _(k):
        transform(k)

    @pl.loop(0, steps)
    def _(k):
        pass_on(k)

        @pl.when(k + ahead < steps)
        def _():
            transform(k + ahead)

        @pl.when(k >= 1)
        def _():
            finish(k - 1)

    finish(steps - 1)

    lane = lax.broadcasted_iota(jnp.int32, gram_send.shape, 1)
    sums = jnp.zeros(gram_send.shape, jnp.float32)
    for n in range(4):
        sums = jnp.where(lane == n, jnp.sum(acc[n], axis=1, keepdims=True), sums)
    gram_send[...] = sums

    def gram_copy(n):
        i, j, x, y = peers[n]
        return pltpu.make_async_remote_copy(
            src_ref=gram_send, dst_ref=gram_recv.at[n],
            send_sem=gram_send_sem.at[n], recv_sem=gram_recv_sem.at[n],
            device_id=(x, y, ta), device_id_type=MESH,
        )

    for n in range(len(peers)):
        gram_copy(n).start()

    @pl.loop(0, steps)
    def _(k):
        for half in range(2):
            for block in range(SEGMENT_NUMBER):
                @pl.when(reaches(ta, block))
                def _():
                    first_copy(half, k, block).wait_send()
            second_copy(half, k).wait_send()

    @pl.loop(max(steps - slots, 0), steps)
    def _(k):
        for half in range(2):
            write(half, k).wait()

    total = sums
    for n in range(len(peers)):
        gram_copy(n).wait()
        total = total + gram_recv[n]
    row = lax.broadcasted_iota(jnp.int32, (8, 128), 0)
    lane = lax.broadcasted_iota(jnp.int32, (8, 128), 1)
    pick = jnp.zeros((8, 128), jnp.float32)
    for r, n, sign in ((0, 0, 1.0), (2, 2, 1.0), (3, 3, 1.0), (4, 2, 1.0), (5, 3, -1.0), (6, 1, 1.0)):
        pick = jnp.where((row == r) & (lane == n), sign, pick)
    gram_ref[...] = gram_scale * lax.dot_general(
        pick, total, (((1,), (1,)), ((), ())),
        precision=lax.Precision.HIGHEST, preferred_element_type=jnp.float32,
    )


def kernel_on_device(snapshots, quad_weights, spectral_indices):
    record, variables, points = snapshots.shape
    groups = lax.axis_size("ta")
    npx, npy = lax.axis_size("px"), lax.axis_size("py")
    modes = spectral_indices.shape[0] // groups
    unit = 2 * modes
    pieces = 2
    width = points // (2 * pieces)
    tile = min(512, width)
    steps = variables * pieces
    slots = 2
    rows = groups * SEGMENT_NUMBER * unit
    bf16, f32 = jnp.bfloat16, jnp.float32
    peers = npx * npy - 1
    spectra, gram = pl.pallas_call(
        functools.partial(
            window_kernel, pieces, width, tile, 1.0 / (points * npx * npy * variables)),
        out_shape=(
            jax.ShapeDtypeStruct((modes, SEGMENT_NUMBER, variables, 2, points), f32),
            jax.ShapeDtypeStruct((SEGMENT_NUMBER * SEGMENT_NUMBER * 2, modes), f32),
        ),
        in_specs=[
            pl.BlockSpec(memory_space=pl.ANY),
            pl.BlockSpec(memory_space=pltpu.VMEM),
            pl.BlockSpec(memory_space=pltpu.SMEM),
        ],
        out_specs=(
            pl.BlockSpec(memory_space=pl.ANY),
            pl.BlockSpec(memory_space=pltpu.VMEM),
        ),
        scratch_shapes=[
            pltpu.VMEM((variables, record, points), bf16),
            pltpu.VMEM((rows, record), bf16),
            pltpu.VMEM((2, steps, SEGMENT_NUMBER, 2 * unit, width), f32),
            pltpu.VMEM((1, points), f32),
            pltpu.VMEM((2, steps, SEGMENT_NUMBER, 2 * unit, width), bf16),
            pltpu.VMEM((2, steps, SEGMENT_NUMBER, 2 * unit, width), bf16),
            pltpu.VMEM((2, steps, SEGMENT_NUMBER * unit, width), bf16),
            pltpu.VMEM((2, steps, SEGMENT_NUMBER * unit, width), bf16),
            pltpu.VMEM((slots, 2, modes, SEGMENT_NUMBER, 2, width), f32),
            pltpu.VMEM((4, modes, 128), f32),
            pltpu.VMEM((modes, 128), f32),
            pltpu.VMEM((peers, modes, 128), f32),
            pltpu.SemaphoreType.DMA((variables,)),
            pltpu.SemaphoreType.DMA((2, steps, SEGMENT_NUMBER)),
            pltpu.SemaphoreType.DMA((2, steps, SEGMENT_NUMBER)),
            pltpu.SemaphoreType.DMA((2, steps)),
            pltpu.SemaphoreType.DMA((2, steps)),
            pltpu.SemaphoreType.DMA((slots, 2)),
            pltpu.SemaphoreType.DMA((peers,)),
            pltpu.SemaphoreType.DMA((peers,)),
        ],
        compiler_params=pltpu.CompilerParams(
            collective_id=0, has_side_effects=True, vmem_limit_bytes=60 * 1024 * 1024),
        name="window_transform",
    )(snapshots.transpose(1, 0, 2), quad_weights.reshape(1, points), spectral_indices)
    gram = gram.reshape(SEGMENT_NUMBER, SEGMENT_NUMBER, 2, modes)
    return spectra.transpose(0, 1, 3, 2, 4), gram.transpose(3, 0, 1, 2)


def solution(mesh):
    square = mesh.shape["ta"] == len(POSITIONS)
    return jax.shard_map(
        kernel_on_device if square else plain_on_device,
        mesh=mesh,
        in_specs=(P("ta", None, ("px", "py")), P(("px", "py")), P()),
        out_specs=(P("ta", None, None, None, ("px", "py")), P("ta", None, None, None)),
        check_vma=False,
    )
```

```python
import functools
import math

import jax
import jax.numpy as jnp
from jax import lax
from jax.experimental import pallas as pl
from jax.experimental.pallas import tpu as pltpu
from jax.sharding import PartitionSpec as P

VARS = 5
BLK = 256
HOP = 128
SEGMENT_NUMBER = 2
RETAINED_MODES = 32

MESH = pl.DeviceIdType.MESH
HALF_NEIGHBOUR = (1, 2)
POSITIONS = (0, 1, 3, 2)
SENT_AT = ((1, 2), (2, 3))
PASSED_AT = (3, 1)
RECEIVED = ((0, 1), (1, 0))


def make_rotation_multipliers(spectral_indices, temporal_locations):
    segment_beginnings = jnp.arange(SEGMENT_NUMBER, dtype=jnp.int32) * HOP
    segment_shifts = temporal_locations[None, :] - segment_beginnings[:, None]
    inside = (segment_shifts >= 0) & (segment_shifts < BLK)
    window = 0.5 - 0.5 * jnp.cos(2.0 * math.pi * segment_shifts.astype(jnp.float32) / BLK)
    window = jnp.where(inside, window, jnp.float32(0.0)) / jnp.sqrt(jnp.float32(3.0 * BLK / 8.0))
    phases = jnp.mod(spectral_indices[:, None, None] * segment_shifts[None, :, :], BLK)
    angles = 2.0 * math.pi * phases.astype(jnp.float32) / BLK
    real_part = jnp.cos(angles) * window[None]
    imag_part = -jnp.sin(angles) * window[None]
    gathered_segments = jnp.stack([real_part, imag_part], axis=2)
    return gathered_segments.reshape(
        RETAINED_MODES * SEGMENT_NUMBER * 2, temporal_locations.shape[0]
    ).astype(jnp.bfloat16)


def gram_terms(spectra):
    flat = spectra.reshape(spectra.shape[0], 2 * SEGMENT_NUMBER, -1)
    inner = jnp.einsum("fam,fbm->fab", flat, flat, precision=lax.Precision.HIGHEST)
    inner = inner.reshape(spectra.shape[0], SEGMENT_NUMBER, 2, SEGMENT_NUMBER, 2)
    real_part = inner[:, :, 0, :, 0] + inner[:, :, 1, :, 1]
    imag_part = inner[:, :, 0, :, 1] - inner[:, :, 1, :, 0]
    return jnp.stack([real_part, imag_part], axis=-1)


def plain_on_device(snapshots, quad_weights, spectral_indices):
    record_length = snapshots.shape[0]
    point_count = snapshots.shape[2]
    groups = lax.axis_size("ta")
    temporal_locations = lax.axis_index("ta") * record_length + jnp.arange(
        record_length, dtype=jnp.int32
    )
    rotation_multipliers = make_rotation_multipliers(spectral_indices, temporal_locations)
    flat_snapshots = snapshots.reshape(record_length, VARS * point_count)
    raw = lax.psum_scatter(
        jnp.dot(rotation_multipliers, flat_snapshots, preferred_element_type=jnp.float32),
        "ta",
        scatter_dimension=0,
        tiled=True,
    )
    raw = raw.reshape(RETAINED_MODES // groups, SEGMENT_NUMBER, 2, VARS, point_count)
    spectra = raw * jnp.sqrt(quad_weights)
    summed = lax.psum(gram_terms(spectra), ("px", "py"))
    total_points = point_count * lax.axis_size("px") * lax.axis_size("py")
    gram = summed / jnp.float32(total_points * VARS)
    return (spectra, gram)


def window_kernel(
    pieces, width, tile, gram_scale,
    snap_hbm, weight_hbm, index_hbm, out_ref, gram_ref,
    snap, index_ref, weight_ref, twiddle, kept, root, send1, recv1, send2, recv2, acc, gram_send, gram_recv,
    load_sem, index_sem, weight_sem, send1_sem, recv1_sem, send2_sem, recv2_sem, gram_send_sem, gram_recv_sem,
):
    px, py, ta = lax.axis_index("px"), lax.axis_index("py"), lax.axis_index("ta")
    npx, npy = lax.axis_size("px"), lax.axis_size("py")
    variables, record, points = snap_hbm.shape
    modes = out_ref.shape[0]
    unit = 2 * modes
    steps = variables * pieces
    neighbours = [jnp.bitwise_xor(ta, flip) for flip in HALF_NEIGHBOUR]

    def load(variable):
        return pltpu.make_async_copy(snap_hbm.at[variable], snap.at[variable], load_sem.at[variable])

    index_copy = pltpu.make_async_copy(index_hbm, index_ref, index_sem)
    weight_copy = pltpu.make_async_copy(weight_hbm, weight_ref, weight_sem)
    index_copy.start()
    for variable in range(variables):
        load(variable).start()
    weight_copy.start()

    peers = [
        (i, j, lax.rem(px + i, npx), lax.rem(py + j, npy))
        for i in range(npx) for j in range(npy) if i + j > 0
    ]
    barrier = pltpu.get_barrier_semaphore()
    for neighbour in neighbours:
        pl.semaphore_signal(barrier, inc=1, device_id=(px, py, neighbour), device_id_type=MESH)
    for _, _, x, y in peers:
        pl.semaphore_signal(barrier, inc=1, device_id=(x, y, ta), device_id_type=MESH)

    def reaches(group, block):
        first = group * record
        return (first < block * HOP + BLK) & (first + record > block * HOP)

    sublane = lax.broadcasted_iota(jnp.int32, (modes, record), 0)
    moment = lax.broadcasted_iota(jnp.int32, (modes, record), 1) + ta * record
    shifts, windows = [], []
    for block in range(SEGMENT_NUMBER):
        shift = moment - block * HOP
        inside = (shift >= 0) & (shift < BLK)
        hann = 0.5 - 0.5 * jnp.cos((2.0 * math.pi / BLK) * shift.astype(jnp.float32))
        shifts.append(shift)
        windows.append(jnp.where(inside, hann, 0.0) / math.sqrt(3.0 * BLK / 8.0))
    index_copy.wait()
    for position, flip in enumerate(POSITIONS):
        owner = jnp.bitwise_xor(ta, flip)
        bins = jnp.zeros((modes, record), jnp.int32)
        for f in range(modes):
            bins = jnp.where(sublane == f, index_ref[owner * modes + f], bins)
        for block in range(SEGMENT_NUMBER):
            shift, hann = shifts[block], windows[block]
            angle = (2.0 * math.pi / BLK) * jnp.bitwise_and(bins * shift, BLK - 1).astype(jnp.float32)
            rows = jnp.concatenate([jnp.cos(angle) * hann, -jnp.sin(angle) * hann], axis=0)
            at = (position * SEGMENT_NUMBER + block) * unit
            twiddle[at:at + unit, :] = rows.astype(jnp.bfloat16)
    acc[...] = jnp.zeros_like(acc)

    pl.semaphore_wait(barrier, len(neighbours) + len(peers))

    def target(half):
        return (px, py, neighbours[half])

    def first_copy(half, k, block):
        return pltpu.make_async_remote_copy(
            src_ref=send1.at[half, k, block], dst_ref=recv1.at[half, k, block],
            send_sem=send1_sem.at[half, k, block], recv_sem=recv1_sem.at[half, k, block],
            device_id=target(half), device_id_type=MESH,
        )

    def second_copy(half, k):
        return pltpu.make_async_remote_copy(
            src_ref=send2.at[half, k], dst_ref=recv2.at[half, k],
            send_sem=send2_sem.at[half, k], recv_sem=recv2_sem.at[half, k],
            device_id=target(1 - half), device_id_type=MESH,
        )

    def columns(half, k, at):
        start = lax.rem(k, pieces) * (2 * width) + half * width + at
        return pl.ds(pl.multiple_of(start, 128), tile)

    def transform(k):
        variable = k // pieces

        @pl.when(lax.rem(k, pieces) == 0)
        def _():
            load(variable).wait()

        for half in range(2):
            @pl.loop(0, width // tile)
            def _(i):
                at = pl.multiple_of(i * tile, tile)
                here = pl.ds(at, tile)
                product = jnp.dot(
                    twiddle[...], snap[variable, :, columns(half, k, at)],
                    preferred_element_type=jnp.float32,
                )

                def part(position, block):
                    first = (position * SEGMENT_NUMBER + block) * unit
                    return product[first:first + unit, :]

                for block in range(SEGMENT_NUMBER):
                    for place, position in enumerate(SENT_AT[half]):
                        send1[half, k, block, place * unit:(place + 1) * unit, here] = part(
                            position, block).astype(jnp.bfloat16)
                    kept[half, k, block, 0:unit, here] = part(0, block)
                    kept[half, k, block, unit:2 * unit, here] = part(PASSED_AT[half], block)

            for block in range(SEGMENT_NUMBER):
                @pl.when(reaches(ta, block))
                def _():
                    first_copy(half, k, block).start()

    def pass_on(k):
        for half in range(2):
            own, other = RECEIVED[half]
            for block in range(SEGMENT_NUMBER):
                came = reaches(neighbours[half], block)

                @pl.when(came)
                def _():
                    first_copy(half, k, block).wait_recv()

                @pl.when(jnp.logical_not(came))
                def _():
                    recv1[half, k, block] = jnp.zeros(recv1.shape[3:], jnp.bfloat16)

            @pl.loop(0, width // tile)
            def _(i):
                here = pl.ds(pl.multiple_of(i * tile, tile), tile)
                for block in range(SEGMENT_NUMBER):
                    arrived = recv1[half, k, block, other * unit:(other + 1) * unit, here]
                    total = kept[half, k, block, unit:2 * unit, here] + arrived.astype(jnp.float32)
                    send2[half, k, block * unit:(block + 1) * unit, here] = total.astype(jnp.bfloat16)

            second_copy(half, k).start()

    def weighted(half, k, i):
        own, _ = RECEIVED[half]
        at = pl.multiple_of(i * tile, tile)
        here = pl.ds(at, tile)
        weight = root[:, columns(half, k, at)]
        parts = []
        for block in range(SEGMENT_NUMBER):
            first = recv1[half, k, block, own * unit:(own + 1) * unit, here]
            second = recv2[half, k, block * unit:(block + 1) * unit, here]
            total = kept[half, k, block, 0:unit, here] + (
                first.astype(jnp.float32) + second.astype(jnp.float32))
            total = total * weight
            parts.append((total[:modes], total[modes:]))
        return parts

    def add_terms(parts):
        (r0, i0), (r1, i1) = parts
        terms = (r0 * r0 + i0 * i0, r1 * r1 + i1 * i1, r0 * r1 + i0 * i1, r0 * i1 - i0 * r1)
        for n, term in enumerate(terms):
            lanes = [term[:, c:c + 128] for c in range(0, tile, 128)]
            acc[n] += functools.reduce(jnp.add, lanes)

    def store(half, k, i, parts):
        here = columns(half, k, pl.multiple_of(i * tile, tile))
        for block, both in enumerate(parts):
            for c in range(2):
                out_ref[:, block, k // pieces, c, here] = both[c]

    def finish(k):
        for half in range(2):
            second_copy(half, k).wait_recv()

            @pl.loop(0, width // tile)
            def _(i):
                parts = weighted(half, k, i)
                add_terms(parts)
                store(half, k, i, parts)

    ahead = min(2, steps)

    @pl.loop(0, ahead)
    def _(k):
        transform(k)

    weight_copy.wait()
    root[...] = jnp.sqrt(weight_ref[...])

    @pl.loop(0, steps)
    def _(k):
        pass_on(k)

        @pl.when(k + ahead < steps)
        def _():
            transform(k + ahead)

        @pl.when(k >= 1)
        def _():
            finish(k - 1)

    for half in range(2):
        second_copy(half, steps - 1).wait_recv()

        @pl.loop(0, width // tile)
        def _(i):
            add_terms(weighted(half, steps - 1, i))

    lane = lax.broadcasted_iota(jnp.int32, gram_send.shape, 1)
    sums = jnp.zeros(gram_send.shape, jnp.float32)
    for n in range(4):
        sums = jnp.where(lane == n, jnp.sum(acc[n], axis=1, keepdims=True), sums)
    gram_send[...] = sums

    def gram_copy(n):
        i, j, x, y = peers[n]
        return pltpu.make_async_remote_copy(
            src_ref=gram_send, dst_ref=gram_recv.at[n],
            send_sem=gram_send_sem.at[n], recv_sem=gram_recv_sem.at[n],
            device_id=(x, y, ta), device_id_type=MESH,
        )

    for n in range(len(peers)):
        gram_copy(n).start()

    for half in range(2):
        @pl.loop(0, width // tile)
        def _(i):
            store(half, steps - 1, i, weighted(half, steps - 1, i))

    @pl.loop(0, steps)
    def _(k):
        for half in range(2):
            for block in range(SEGMENT_NUMBER):
                @pl.when(reaches(ta, block))
                def _():
                    first_copy(half, k, block).wait_send()
            second_copy(half, k).wait_send()

    total = sums
    for n in range(len(peers)):
        gram_copy(n).wait()
        total = total + gram_recv[n]
    row = lax.broadcasted_iota(jnp.int32, (8, 128), 0)
    lane = lax.broadcasted_iota(jnp.int32, (8, 128), 1)
    pick = jnp.zeros((8, 128), jnp.float32)
    for r, n, sign in ((0, 0, 1.0), (2, 2, 1.0), (3, 3, 1.0), (4, 2, 1.0), (5, 3, -1.0), (6, 1, 1.0)):
        pick = jnp.where((row == r) & (lane == n), sign, pick)
    gram_ref[...] = gram_scale * lax.dot_general(
        pick, total, (((1,), (1,)), ((), ())),
        precision=lax.Precision.HIGHEST, preferred_element_type=jnp.float32,
    )


def kernel_on_device(snapshots, quad_weights, spectral_indices):
    record, variables, points = snapshots.shape
    groups = lax.axis_size("ta")
    npx, npy = lax.axis_size("px"), lax.axis_size("py")
    modes = spectral_indices.shape[0] // groups
    unit = 2 * modes
    pieces = 4
    width = points // (2 * pieces)
    tile = math.gcd(512, width)
    steps = variables * pieces
    rows = groups * SEGMENT_NUMBER * unit
    bf16, f32 = jnp.bfloat16, jnp.float32
    peers = npx * npy - 1
    spectra, gram = pl.pallas_call(
        functools.partial(
            window_kernel, pieces, width, tile, 1.0 / (points * npx * npy * variables)),
        out_shape=(
            jax.ShapeDtypeStruct((modes, SEGMENT_NUMBER, variables, 2, points), f32),
            jax.ShapeDtypeStruct((SEGMENT_NUMBER * SEGMENT_NUMBER * 2, modes), f32),
        ),
        in_specs=[
            pl.BlockSpec(memory_space=pltpu.HBM),
            pl.BlockSpec(memory_space=pltpu.HBM),
            pl.BlockSpec(memory_space=pltpu.HBM),
        ],
        out_specs=(
            pl.BlockSpec(memory_space=pltpu.VMEM),
            pl.BlockSpec(memory_space=pltpu.VMEM),
        ),
        scratch_shapes=[
            pltpu.VMEM((variables, record, points), bf16),
            pltpu.SMEM(spectral_indices.shape, jnp.int32),
            pltpu.VMEM((1, points), f32),
            pltpu.VMEM((rows, record), bf16),
            pltpu.VMEM((2, steps, SEGMENT_NUMBER, 2 * unit, width), f32),
            pltpu.VMEM((1, points), f32),
            pltpu.VMEM((2, steps, SEGMENT_NUMBER, 2 * unit, width), bf16),
            pltpu.VMEM((2, steps, SEGMENT_NUMBER, 2 * unit, width), bf16),
            pltpu.VMEM((2, steps, SEGMENT_NUMBER * unit, width), bf16),
            pltpu.VMEM((2, steps, SEGMENT_NUMBER * unit, width), bf16),
            pltpu.VMEM((4, modes, 128), f32),
            pltpu.VMEM((modes, 128), f32),
            pltpu.VMEM((peers, modes, 128), f32),
            pltpu.SemaphoreType.DMA((variables,)),
            pltpu.SemaphoreType.DMA,
            pltpu.SemaphoreType.DMA,
            pltpu.SemaphoreType.DMA((2, steps, SEGMENT_NUMBER)),
            pltpu.SemaphoreType.DMA((2, steps, SEGMENT_NUMBER)),
            pltpu.SemaphoreType.DMA((2, steps)),
            pltpu.SemaphoreType.DMA((2, steps)),
            pltpu.SemaphoreType.DMA((peers,)),
            pltpu.SemaphoreType.DMA((peers,)),
        ],
        compiler_params=pltpu.CompilerParams(
            collective_id=0, has_side_effects=True, vmem_limit_bytes=44 * 1024 * 1024),
        name="window_transform",
    )(*(
        pltpu.with_memory_space_constraint(a, pltpu.HBM)
        for a in (snapshots.transpose(1, 0, 2), quad_weights.reshape(1, points), spectral_indices)
    ))
    gram = gram.reshape(SEGMENT_NUMBER, SEGMENT_NUMBER, 2, modes)
    return spectra.transpose(0, 1, 3, 2, 4), gram.transpose(3, 0, 1, 2)


def solution(mesh):
    square = mesh.shape["ta"] == len(POSITIONS)
    return jax.shard_map(
        kernel_on_device if square else plain_on_device,
        mesh=mesh,
        in_specs=(P("ta", None, ("px", "py")), P(("px", "py")), P()),
        out_specs=(P("ta", None, None, None, ("px", "py")), P("ta", None, None, None)),
        check_vma=False,
    )
```

```python
import functools
import math

import jax
import jax.numpy as jnp
from jax import lax
from jax.experimental import pallas as pl
from jax.experimental.pallas import tpu as pltpu
from jax.sharding import PartitionSpec as P

VARS = 5
BLK = 256
HOP = 128
SEGMENT_NUMBER = 2
RETAINED_MODES = 32

MESH = pl.DeviceIdType.MESH
HALF_NEIGHBOUR = (1, 2)
POSITIONS = (0, 1, 3, 2)
SENT_AT = ((1, 2), (2, 3))
PASSED_AT = (3, 1)
RECEIVED = ((0, 1), (1, 0))


def make_rotation_multipliers(spectral_indices, temporal_locations):
    segment_beginnings = jnp.arange(SEGMENT_NUMBER, dtype=jnp.int32) * HOP
    segment_shifts = temporal_locations[None, :] - segment_beginnings[:, None]
    inside = (segment_shifts >= 0) & (segment_shifts < BLK)
    window = 0.5 - 0.5 * jnp.cos(2.0 * math.pi * segment_shifts.astype(jnp.float32) / BLK)
    window = jnp.where(inside, window, jnp.float32(0.0)) / jnp.sqrt(jnp.float32(3.0 * BLK / 8.0))
    phases = jnp.mod(spectral_indices[:, None, None] * segment_shifts[None, :, :], BLK)
    angles = 2.0 * math.pi * phases.astype(jnp.float32) / BLK
    real_part = jnp.cos(angles) * window[None]
    imag_part = -jnp.sin(angles) * window[None]
    gathered_segments = jnp.stack([real_part, imag_part], axis=2)
    return gathered_segments.reshape(
        RETAINED_MODES * SEGMENT_NUMBER * 2, temporal_locations.shape[0]
    ).astype(jnp.bfloat16)


def gram_terms(spectra):
    flat = spectra.reshape(spectra.shape[0], 2 * SEGMENT_NUMBER, -1)
    inner = jnp.einsum("fam,fbm->fab", flat, flat, precision=lax.Precision.HIGHEST)
    inner = inner.reshape(spectra.shape[0], SEGMENT_NUMBER, 2, SEGMENT_NUMBER, 2)
    real_part = inner[:, :, 0, :, 0] + inner[:, :, 1, :, 1]
    imag_part = inner[:, :, 0, :, 1] - inner[:, :, 1, :, 0]
    return jnp.stack([real_part, imag_part], axis=-1)


def plain_on_device(snapshots, quad_weights, spectral_indices):
    record_length = snapshots.shape[0]
    point_count = snapshots.shape[2]
    groups = lax.axis_size("ta")
    temporal_locations = lax.axis_index("ta") * record_length + jnp.arange(
        record_length, dtype=jnp.int32
    )
    rotation_multipliers = make_rotation_multipliers(spectral_indices, temporal_locations)
    flat_snapshots = snapshots.reshape(record_length, VARS * point_count)
    raw = lax.psum_scatter(
        jnp.dot(rotation_multipliers, flat_snapshots, preferred_element_type=jnp.float32),
        "ta",
        scatter_dimension=0,
        tiled=True,
    )
    raw = raw.reshape(RETAINED_MODES // groups, SEGMENT_NUMBER, 2, VARS, point_count)
    spectra = raw * jnp.sqrt(quad_weights)
    summed = lax.psum(gram_terms(spectra), ("px", "py"))
    total_points = point_count * lax.axis_size("px") * lax.axis_size("py")
    gram = summed / jnp.float32(total_points * VARS)
    return (spectra, gram)


def sine_of_turn(m):
    quarter = BLK // 4
    r = jnp.bitwise_and(m + quarter, BLK - 1) - quarter
    r = jnp.where(r > quarter, BLK // 2 - r, r)
    x = r.astype(jnp.float32) * (2.0 * math.pi / BLK)
    y = x * x
    total = jnp.full_like(x, -1.0 / math.factorial(11))
    for n in (9, 7, 5, 3, 1):
        total = total * y + (1.0 if n % 4 == 1 else -1.0) / math.factorial(n)
    return total * x


def window_kernel(
    pieces, width, tile, gram_scale,
    snap_hbm, weight_hbm, index_hbm, out_ref, gram_ref,
    snap, index_ref, weight_ref, twiddle, kept, root, send1, recv1, send2, recv2, acc, gram_send, gram_recv,
    load_sem, index_sem, weight_sem, send1_sem, recv1_sem, send2_sem, recv2_sem, gram_send_sem, gram_recv_sem,
):
    px, py, ta = lax.axis_index("px"), lax.axis_index("py"), lax.axis_index("ta")
    npx, npy = lax.axis_size("px"), lax.axis_size("py")
    variables, record, points = snap_hbm.shape
    modes = out_ref.shape[0]
    unit = 2 * modes
    steps = variables * pieces
    neighbours = [jnp.bitwise_xor(ta, flip) for flip in HALF_NEIGHBOUR]

    def load(variable):
        return pltpu.make_async_copy(snap_hbm.at[variable], snap.at[variable], load_sem.at[variable])

    index_copy = pltpu.make_async_copy(index_hbm, index_ref, index_sem)
    weight_copy = pltpu.make_async_copy(weight_hbm, weight_ref, weight_sem)
    index_copy.start()
    for variable in range(variables):
        load(variable).start()
    weight_copy.start()

    peers = [
        (i, j, lax.rem(px + i, npx), lax.rem(py + j, npy))
        for i in range(npx) for j in range(npy) if i + j > 0
    ]
    barrier = pltpu.get_barrier_semaphore()
    for neighbour in neighbours:
        pl.semaphore_signal(barrier, inc=1, device_id=(px, py, neighbour), device_id_type=MESH)
    for _, _, x, y in peers:
        pl.semaphore_signal(barrier, inc=1, device_id=(x, y, ta), device_id_type=MESH)

    def reaches(group, block):
        first = group * record
        return (first < block * HOP + BLK) & (first + record > block * HOP)

    sublane = lax.broadcasted_iota(jnp.int32, (modes, record), 0)
    moment = lax.broadcasted_iota(jnp.int32, (modes, record), 1) + ta * record
    shifts, windows = [], []
    for block in range(SEGMENT_NUMBER):
        shift = moment - block * HOP
        inside = (shift >= 0) & (shift < BLK)
        hann = 0.5 - 0.5 * sine_of_turn(shift + BLK // 4)
        shifts.append(shift)
        windows.append(jnp.where(inside, hann, 0.0) / math.sqrt(3.0 * BLK / 8.0))
    index_copy.wait()
    for position, flip in enumerate(POSITIONS):
        owner = jnp.bitwise_xor(ta, flip)
        bins = jnp.zeros((modes, record), jnp.int32)
        for f in range(modes):
            bins = jnp.where(sublane == f, index_ref[owner * modes + f], bins)
        for block in range(SEGMENT_NUMBER):
            shift, hann = shifts[block], windows[block]
            phase = bins * shift
            rows = jnp.concatenate(
                [sine_of_turn(phase + BLK // 4) * hann, -sine_of_turn(phase) * hann], axis=0)
            at = (position * SEGMENT_NUMBER + block) * unit
            twiddle[at:at + unit, :] = rows.astype(jnp.bfloat16)
    acc[...] = jnp.zeros_like(acc)

    pl.semaphore_wait(barrier, len(neighbours) + len(peers))

    def target(half):
        return (px, py, neighbours[half])

    def first_copy(half, k, block):
        return pltpu.make_async_remote_copy(
            src_ref=send1.at[half, k, block], dst_ref=recv1.at[half, k, block],
            send_sem=send1_sem.at[half, k, block], recv_sem=recv1_sem.at[half, k, block],
            device_id=target(half), device_id_type=MESH,
        )

    def second_copy(half, k):
        return pltpu.make_async_remote_copy(
            src_ref=send2.at[half, k], dst_ref=recv2.at[half, k],
            send_sem=send2_sem.at[half, k], recv_sem=recv2_sem.at[half, k],
            device_id=target(1 - half), device_id_type=MESH,
        )

    def columns(half, k, at):
        start = lax.rem(k, pieces) * (2 * width) + half * width + at
        return pl.ds(pl.multiple_of(start, 128), tile)

    def transform(k):
        variable = k // pieces

        @pl.when(lax.rem(k, pieces) == 0)
        def _():
            load(variable).wait()

        for half in range(2):
            @pl.loop(0, width // tile)
            def _(i):
                at = pl.multiple_of(i * tile, tile)
                here = pl.ds(at, tile)
                product = jnp.dot(
                    twiddle[...], snap[variable, :, columns(half, k, at)],
                    preferred_element_type=jnp.float32,
                )

                def part(position, block):
                    first = (position * SEGMENT_NUMBER + block) * unit
                    return product[first:first + unit, :]

                for block in range(SEGMENT_NUMBER):
                    for place, position in enumerate(SENT_AT[half]):
                        send1[half, k, block, place * unit:(place + 1) * unit, here] = part(
                            position, block).astype(jnp.bfloat16)
                    kept[half, k, block, 0:unit, here] = part(0, block)
                    kept[half, k, block, unit:2 * unit, here] = part(PASSED_AT[half], block)

            for block in range(SEGMENT_NUMBER):
                @pl.when(reaches(ta, block))
                def _():
                    first_copy(half, k, block).start()

    def pass_on(k):
        for half in range(2):
            own, other = RECEIVED[half]
            for block in range(SEGMENT_NUMBER):
                came = reaches(neighbours[half], block)

                @pl.when(came)
                def _():
                    first_copy(half, k, block).wait_recv()

                @pl.when(jnp.logical_not(came))
                def _():
                    recv1[half, k, block] = jnp.zeros(recv1.shape[3:], jnp.bfloat16)

            @pl.loop(0, width // tile)
            def _(i):
                here = pl.ds(pl.multiple_of(i * tile, tile), tile)
                for block in range(SEGMENT_NUMBER):
                    arrived = recv1[half, k, block, other * unit:(other + 1) * unit, here]
                    total = kept[half, k, block, unit:2 * unit, here] + arrived.astype(jnp.float32)
                    send2[half, k, block * unit:(block + 1) * unit, here] = total.astype(jnp.bfloat16)

            second_copy(half, k).start()

    def weighted(half, k, i):
        own, _ = RECEIVED[half]
        at = pl.multiple_of(i * tile, tile)
        here = pl.ds(at, tile)
        weight = root[:, columns(half, k, at)]
        parts = []
        for block in range(SEGMENT_NUMBER):
            first = recv1[half, k, block, own * unit:(own + 1) * unit, here]
            second = recv2[half, k, block * unit:(block + 1) * unit, here]
            total = kept[half, k, block, 0:unit, here] + (
                first.astype(jnp.float32) + second.astype(jnp.float32))
            total = total * weight
            parts.append((total[:modes], total[modes:]))
        return parts

    def add_terms(parts):
        (r0, i0), (r1, i1) = parts
        terms = (r0 * r0 + i0 * i0, r1 * r1 + i1 * i1, r0 * r1 + i0 * i1, r0 * i1 - i0 * r1)
        for n, term in enumerate(terms):
            lanes = [term[:, c:c + 128] for c in range(0, tile, 128)]
            acc[n] += functools.reduce(jnp.add, lanes)

    def store(half, k, i, parts):
        here = columns(half, k, pl.multiple_of(i * tile, tile))
        for block, both in enumerate(parts):
            for c in range(2):
                out_ref[:, block, k // pieces, c, here] = both[c]

    def finish(k):
        for half in range(2):
            second_copy(half, k).wait_recv()

            @pl.loop(0, width // tile)
            def _(i):
                parts = weighted(half, k, i)
                add_terms(parts)
                store(half, k, i, parts)

    ahead = min(2, steps)

    @pl.loop(0, ahead)
    def _(k):
        transform(k)

    weight_copy.wait()
    root[...] = jnp.sqrt(weight_ref[...])

    @pl.loop(0, steps)
    def _(k):
        pass_on(k)

        @pl.when(k + ahead < steps)
        def _():
            transform(k + ahead)

        @pl.when(k >= 1)
        def _():
            finish(k - 1)

    for half in range(2):
        second_copy(half, steps - 1).wait_recv()

        @pl.loop(0, width // tile)
        def _(i):
            add_terms(weighted(half, steps - 1, i))

    lane = lax.broadcasted_iota(jnp.int32, gram_send.shape, 1)
    sums = jnp.zeros(gram_send.shape, jnp.float32)
    for n in range(4):
        sums = jnp.where(lane == n, jnp.sum(acc[n], axis=1, keepdims=True), sums)
    gram_send[...] = sums

    def gram_copy(n):
        i, j, x, y = peers[n]
        return pltpu.make_async_remote_copy(
            src_ref=gram_send, dst_ref=gram_recv.at[n],
            send_sem=gram_send_sem.at[n], recv_sem=gram_recv_sem.at[n],
            device_id=(x, y, ta), device_id_type=MESH,
        )

    for n in range(len(peers)):
        gram_copy(n).start()

    for half in range(2):
        @pl.loop(0, width // tile)
        def _(i):
            store(half, steps - 1, i, weighted(half, steps - 1, i))

    @pl.loop(0, steps)
    def _(k):
        for half in range(2):
            for block in range(SEGMENT_NUMBER):
                @pl.when(reaches(ta, block))
                def _():
                    first_copy(half, k, block).wait_send()
            second_copy(half, k).wait_send()

    total = sums
    for n in range(len(peers)):
        gram_copy(n).wait()
        total = total + gram_recv[n]
    row = lax.broadcasted_iota(jnp.int32, (8, 128), 0)
    lane = lax.broadcasted_iota(jnp.int32, (8, 128), 1)
    pick = jnp.zeros((8, 128), jnp.float32)
    for r, n, sign in ((0, 0, 1.0), (2, 2, 1.0), (3, 3, 1.0), (4, 2, 1.0), (5, 3, -1.0), (6, 1, 1.0)):
        pick = jnp.where((row == r) & (lane == n), sign, pick)
    gram_ref[...] = gram_scale * lax.dot_general(
        pick, total, (((1,), (1,)), ((), ())),
        precision=lax.Precision.HIGHEST, preferred_element_type=jnp.float32,
    )


def kernel_on_device(snapshots, quad_weights, spectral_indices):
    record, variables, points = snapshots.shape
    groups = lax.axis_size("ta")
    npx, npy = lax.axis_size("px"), lax.axis_size("py")
    modes = spectral_indices.shape[0] // groups
    unit = 2 * modes
    pieces = 2
    width = points // (2 * pieces)
    tile = math.gcd(512, width)
    steps = variables * pieces
    rows = groups * SEGMENT_NUMBER * unit
    bf16, f32 = jnp.bfloat16, jnp.float32
    peers = npx * npy - 1
    spectra, gram = pl.pallas_call(
        functools.partial(
            window_kernel, pieces, width, tile, 1.0 / (points * npx * npy * variables)),
        out_shape=(
            jax.ShapeDtypeStruct((modes, SEGMENT_NUMBER, variables, 2, points), f32),
            jax.ShapeDtypeStruct((SEGMENT_NUMBER * SEGMENT_NUMBER * 2, modes), f32),
        ),
        in_specs=[
            pl.BlockSpec(memory_space=pltpu.HBM),
            pl.BlockSpec(memory_space=pltpu.HBM),
            pl.BlockSpec(memory_space=pltpu.HBM),
        ],
        out_specs=(
            pl.BlockSpec(memory_space=pltpu.VMEM),
            pl.BlockSpec(memory_space=pltpu.VMEM),
        ),
        scratch_shapes=[
            pltpu.VMEM((variables, record, points), bf16),
            pltpu.SMEM(spectral_indices.shape, jnp.int32),
            pltpu.VMEM((1, points), f32),
            pltpu.VMEM((rows, record), bf16),
            pltpu.VMEM((2, steps, SEGMENT_NUMBER, 2 * unit, width), f32),
            pltpu.VMEM((1, points), f32),
            pltpu.VMEM((2, steps, SEGMENT_NUMBER, 2 * unit, width), bf16),
            pltpu.VMEM((2, steps, SEGMENT_NUMBER, 2 * unit, width), bf16),
            pltpu.VMEM((2, steps, SEGMENT_NUMBER * unit, width), bf16),
            pltpu.VMEM((2, steps, SEGMENT_NUMBER * unit, width), bf16),
            pltpu.VMEM((4, modes, 128), f32),
            pltpu.VMEM((modes, 128), f32),
            pltpu.VMEM((peers, modes, 128), f32),
            pltpu.SemaphoreType.DMA((variables,)),
            pltpu.SemaphoreType.DMA,
            pltpu.SemaphoreType.DMA,
            pltpu.SemaphoreType.DMA((2, steps, SEGMENT_NUMBER)),
            pltpu.SemaphoreType.DMA((2, steps, SEGMENT_NUMBER)),
            pltpu.SemaphoreType.DMA((2, steps)),
            pltpu.SemaphoreType.DMA((2, steps)),
            pltpu.SemaphoreType.DMA((peers,)),
            pltpu.SemaphoreType.DMA((peers,)),
        ],
        compiler_params=pltpu.CompilerParams(
            collective_id=0, has_side_effects=True, vmem_limit_bytes=44 * 1024 * 1024),
        name="window_transform",
    )(*(
        pltpu.with_memory_space_constraint(a, pltpu.HBM)
        for a in (snapshots.transpose(1, 0, 2), quad_weights.reshape(1, points), spectral_indices)
    ))
    gram = gram.reshape(SEGMENT_NUMBER, SEGMENT_NUMBER, 2, modes)
    return spectra.transpose(0, 1, 3, 2, 4), gram.transpose(3, 0, 1, 2)


def solution(mesh):
    square = mesh.shape["ta"] == len(POSITIONS)
    return jax.shard_map(
        kernel_on_device if square else plain_on_device,
        mesh=mesh,
        in_specs=(P("ta", None, ("px", "py")), P(("px", "py")), P()),
        out_specs=(P("ta", None, None, None, ("px", "py")), P("ta", None, None, None)),
        check_vma=False,
    )
```
